32 devices in a mesh: rep: 8 (over z, x), tp: 4 (over y, core).
Axes of the slice: x: 2, y: 2, z: 4, core: 2. Of those that a mesh axis runs over, the one named last changes fastest.
Arguments:
- q_weight: float32 [5120, 5120], P(('rep', 'tp')), may hold values from -0.078125 to 0.078125
- key_projection_weight: float32 [1024, 5120], P(('rep', 'tp')), may hold values from -0.078125 to 0.078125
- value_projection_weight: float32 [1024, 5120], P(('rep', 'tp')), may hold values from -0.078125 to 0.078125
- tokens: bfloat16 [8192, 5120], P(('rep', 'tp')), may hold values from -6 to 6
Outputs:
- combined_query_key_value: bfloat16 [7168, 5120], P('tp')
- projected: bfloat16 [8192, 7168], P('rep', 'tp')
The draws below stay inside these ranges and needn't reach their ends.
All inputs are finite; a program needn't handle non-finite values.
Results may differ from the reference program's by a relative error of at most 0.0049.
Values may be sent and summed in bfloat16 or wider, within the bound.
A program may use at most 192 MiB of HBM per device.

```python
import jax
import jax.numpy as jnp

MODEL_WIDTH = 5120
HQ = 40
KEY_VALUE_HEADS = 8
HEAD_SIZE = 128
TOKENS = 8192
N_TP = 4


def block_scale(key, shape, cuts, smallest, top_value):
    level, own = 1.0, jax.random.fold_in(key, 6)
    for dim, shards_of in cuts:
        heights = jnp.exp(jax.random.uniform(jax.random.fold_in(own, dim), (shards_of,), jnp.float32, smallest / len(cuts), top_value / len(cuts)))
        level = level * jnp.repeat(heights, shape[dim] // shards_of).reshape([-1 if axis == dim else 1 for axis in range(len(shape))])
    return level


def bell_draw(key, dims, width, bound, shards=(), kind=jnp.bfloat16):
    array = width * jax.random.normal(key, dims, jnp.float32)
    if shards:
        array = array * block_scale(key, dims, shards, -0.22, 0.18)
    return jnp.clip(array, -bound, bound).astype(kind)


def setup_inputs(seed: int = 0) -> dict:
    seeds = jax.random.split(jax.random.key(seed), 5)
    return {
        "q_weight": bell_draw(seeds[0], (HQ * HEAD_SIZE, MODEL_WIDTH), MODEL_WIDTH ** -0.5, 0.078125, ((0, 32),), jnp.float32),
        "key_projection_weight": bell_draw(seeds[1], (KEY_VALUE_HEADS * HEAD_SIZE, MODEL_WIDTH), MODEL_WIDTH ** -0.5, 0.078125, ((0, 32),), jnp.float32),
        "value_projection_weight": bell_draw(seeds[2], (KEY_VALUE_HEADS * HEAD_SIZE, MODEL_WIDTH), MODEL_WIDTH ** -0.5, 0.078125, ((0, 32),), jnp.float32),
        "tokens": bell_draw(seeds[3], (TOKENS, MODEL_WIDTH), 1.0, 6.0, ((0, 32),)),
    }


def reference(q_weight, key_projection_weight, value_projection_weight, tokens):
    blocks = []
    for source in (q_weight, key_projection_weight, value_projection_weight):
        rounded = source.astype(jnp.bfloat16)
        blocks.append(rounded.reshape(N_TP, -1, MODEL_WIDTH))
    combined_query_key_value = jnp.concatenate(blocks, axis=1).reshape(-1, MODEL_WIDTH)
    projected = jnp.dot(tokens, combined_query_key_value.T, preferred_element_type=jnp.float32).astype(jnp.bfloat16)
    return combined_query_key_value, projected
```

```python
import functools

import jax
import jax.numpy as jnp
from jax import lax
from jax.experimental import pallas as pl
from jax.experimental.pallas import tpu as pltpu
from jax.sharding import PartitionSpec as P

MESH = pl.DeviceIdType.MESH
LEAD = 3
Y_LAG = 5


def gather_kernel(
    rep_size, tp_size, q_rows, kv_rows,
    shard, tok, weights, prompts, relay,
    shard_buf, tok_buf, local_sem,
    part_send, part_recv, z_send, z_recv, y_send, y_recv, x_send, x_recv, tok_send, tok_recv,
):
    planes = tp_size
    columns = rep_size // planes
    half = tp_size // 2
    r, t = lax.axis_index("rep"), lax.axis_index("tp")
    plane, column = r // columns, r % columns
    side, core = t // 2, t % 2
    other = (t + half) % tp_size
    partner = t + 1 - 2 * core
    q_chunks = q_rows // kv_rows
    pieces = q_chunks + 2
    count = 2 * pieces
    shards_in_plane = tp_size * columns
    ranks = (t, other)

    def row_of(index, m):
        if m < q_chunks:
            return pl.multiple_of(index * q_rows + m * kv_rows, 8)
        base = shards_in_plane * (q_rows + (m - q_chunks) * kv_rows)
        return pl.multiple_of(base + index * kv_rows, 8)

    def in_weights(at_side, n):
        of_core = core if n < pieces else 1 - core
        return weights.at[pl.ds(row_of(column * tp_size + at_side * 2 + of_core, n % pieces), kv_rows)]

    def in_relay(n):
        return relay.at[pl.ds(n * kv_rows, kv_rows)]

    def in_shard(m):
        return shard.at[pl.ds(m * kv_rows, kv_rows)]

    def place(slot, n):
        return in_weights(side, n) if slot == 0 else in_relay(n)

    def remote(src, dst, send, recv, to_rep, to_tp):
        return pltpu.make_async_remote_copy(
            src_ref=src, dst_ref=dst, send_sem=send, recv_sem=recv,
            device_id=(to_rep, to_tp), device_id_type=MESH,
        )

    def ups(slot):
        k = ranks[slot]
        return (plane >= k) & (plane < planes - 1), (plane <= k) & (plane > 0)

    def x_sends(src, dst):
        for d in range(1, columns):
            to = plane * columns + (column + d) % columns
            remote(src, dst, x_send.at[d - 1], x_recv.at[d - 1], to, t).start()

    def forward(slot, n, src):
        up, down = ups(slot)
        dst = place(slot, n)

        @pl.when(up)
        def _():
            remote(src, dst, z_send.at[slot, 0], z_recv.at[slot, n], r + columns, t).start()

        @pl.when(down)
        def _():
            remote(src, dst, z_send.at[slot, 1], z_recv.at[slot, n], r - columns, t).start()

        if slot == 0:
            x_sends(src, dst)
        else:
            remote(src, in_weights(side, n), y_send.at[0], y_recv.at[n], r, other).start()

    def recv_wait(dst, sem):
        remote(dst, dst, x_send.at[0], sem, r, partner).wait_recv()

    def send_wait(src, sem):
        remote(src, src, sem, x_recv.at[0], r, partner).wait_send()

    def source_step(slot, n):
        @pl.when(plane == ranks[slot])
        def _():
            if n < pieces:
                forward(slot, n, in_shard(n))
            else:
                recv_wait(place(slot, n), part_recv.at[n - pieces])
                forward(slot, n, place(slot, n))

    def relay_step(slot, n):
        @pl.when(plane != ranks[slot])
        def _():
            recv_wait(place(slot, n), z_recv.at[slot, n])
            forward(slot, n, place(slot, n))

    def y_step(n):
        block = in_weights(1 - side, n)
        recv_wait(block, y_recv.at[n])
        x_sends(block, block)

    rows = tok.shape[0]

    def prompt_rows(rank):
        return prompts.at[pl.ds(pl.multiple_of(rank * rows, 8), rows)]

    handler = core == plane % 2
    load_shard = pltpu.make_async_copy(shard, shard_buf, local_sem.at[0])
    load_tok = pltpu.make_async_copy(tok, tok_buf, local_sem.at[1])
    load_shard.start()
    load_tok.start()

    @pl.when(jnp.logical_not(handler))
    def _():
        for m in range(pieces):
            @pl.when(side == plane // 2)
            def _():
                dst = weights.at[pl.ds(row_of(column * tp_size + t, m), kv_rows)]
                remote(in_shard(m), dst, part_send.at[0], part_recv.at[m], r, partner).start()

            @pl.when(side != plane // 2)
            def _():
                remote(in_shard(m), in_relay(pieces + m), part_send.at[0], part_recv.at[m], r, partner).start()

    remote(tok, prompt_rows(t), tok_send.at[0], tok_recv.at[0], r, other).start()
    remote(tok, prompt_rows(t), tok_send.at[1], tok_recv.at[1], r, partner).start()

    for n in range(LEAD):
        source_step(0, n)
        source_step(1, n)

    load_shard.wait()
    load_tok.wait()
    store_tok = pltpu.make_async_copy(tok_buf, prompt_rows(t), local_sem.at[1])
    store_tok.start()

    def store_shard(m):
        dst = weights.at[pl.ds(row_of(column * tp_size + t, m), kv_rows)]
        return pltpu.make_async_copy(shard_buf.at[pl.ds(m * kv_rows, kv_rows)], dst, local_sem.at[2 + m])

    @pl.when(plane == t)
    def _():
        for m in range(pieces):
            store_shard(m).start()

    for n in range(count):
        if n + LEAD < count:
            source_step(0, n + LEAD)
            source_step(1, n + LEAD)
        relay_step(0, n)
        relay_step(1, n)
        if n == Y_LAG:
            recv_wait(prompt_rows(other), tok_recv.at[0])
            remote(prompt_rows(other), prompt_rows(other), tok_send.at[2], tok_recv.at[2], r, partner).start()
        if n >= Y_LAG:
            y_step(n - Y_LAG)
    for n in range(count - Y_LAG, count):
        y_step(n)

    quarter = count * kv_rows
    recv_wait(prompt_rows(partner), tok_recv.at[1])
    recv_wait(prompt_rows((partner + half) % tp_size), tok_recv.at[2])
    for d in range(1, columns):
        recv_wait(weights.at[pl.ds(0, 2 * quarter)], x_recv.at[d - 1])
        send_wait(weights.at[pl.ds(0, 2 * quarter)], x_send.at[d - 1])
    send_wait(relay, y_send.at[0])
    for slot in range(2):
        for way, go in enumerate(ups(slot)):
            @pl.when(go)
            def _():
                send_wait(relay, z_send.at[slot, way])

    @pl.when(jnp.logical_not(handler))
    def _():
        send_wait(shard, part_send.at[0])

    for i in range(3):
        send_wait(tok, tok_send.at[i])
    store_tok.wait()

    @pl.when(plane == t)
    def _():
        for m in range(pieces):
            store_shard(m).wait()


def gather(shard, tok, q_rows, kv_rows):
    rep_size, tp_size = lax.axis_size("rep"), lax.axis_size("tp")
    columns = rep_size // tp_size
    width = shard.shape[1]
    pieces = q_rows // kv_rows + 2
    count = 2 * pieces
    hbm = pl.BlockSpec(memory_space=pltpu.HBM)
    dma = pltpu.SemaphoreType.DMA
    weights, prompts, _ = pl.pallas_call(
        functools.partial(gather_kernel, rep_size, tp_size, q_rows, kv_rows),
        out_shape=(
            jax.ShapeDtypeStruct((rep_size * shard.shape[0], width), shard.dtype),
            jax.ShapeDtypeStruct((tp_size * tok.shape[0], width), tok.dtype),
            jax.ShapeDtypeStruct((count * kv_rows, width), shard.dtype),
        ),
        in_specs=[hbm, hbm],
        out_specs=(hbm, hbm, hbm),
        scratch_shapes=[
            pltpu.VMEM(shard.shape, shard.dtype),
            pltpu.VMEM(tok.shape, tok.dtype),
            dma((2 + pieces,)),
            dma((1,)), dma((pieces,)),
            dma((2, 2)), dma((2, count)),
            dma((1,)), dma((count,)),
            dma((columns - 1,)), dma((columns - 1,)),
            dma((3,)), dma((3,)),
        ],
        compiler_params=pltpu.CompilerParams(has_side_effects=True, vmem_limit_bytes=16 * 2**20),
    )(shard, tok)
    return weights, prompts


def shards(q_weight, key_projection_weight, value_projection_weight, tokens):
    shard = jnp.concatenate(
        [q_weight, key_projection_weight, value_projection_weight], 0
    ).astype(jnp.bfloat16)
    weights, prompts = gather(shard, tokens, q_weight.shape[0], key_projection_weight.shape[0])
    projected = lax.dot_general(
        prompts, weights, (((1,), (1,)), ((), ())), preferred_element_type=jnp.float32
    )
    return weights, projected.astype(jnp.bfloat16)


def solution(mesh):
    spec = P(("rep", "tp"), None)
    return jax.shard_map(
        shards, mesh=mesh, in_specs=(spec,) * 4, out_specs=(P("tp", None), P("rep", "tp")), check_vma=False
    )
```

```python
import functools

import jax
import jax.numpy as jnp
from jax import lax
from jax.experimental import pallas as pl
from jax.experimental.pallas import tpu as pltpu
from jax.sharding import PartitionSpec as P

MESH = pl.DeviceIdType.MESH
LEAD = 3
Y_LAG = 3
TOK_AT = 11
LATE_FIRST = 1
LATE_EVERY = 3


def gather_kernel(
    rep_size, tp_size, q_rows, kv_rows,
    shard, tok, weights, projected,
    prompts, relay, shard_buf, block_buf, result_buf, local_sem, block_sem, result_sem,
    part_send, part_recv, z_send, z_recv, y_send, y_recv, x_send, x_recv, tok_send, tok_recv,
):
    planes = tp_size
    columns = rep_size // planes
    half = tp_size // 2
    r, t = lax.axis_index("rep"), lax.axis_index("tp")
    plane, column = r // columns, r % columns
    side, core = t // 2, t % 2
    other = (t + half) % tp_size
    partner = t + 1 - 2 * core
    q_chunks = q_rows // kv_rows
    pieces = q_chunks + 2
    count = 2 * pieces
    shards_in_plane = tp_size * columns
    ranks = (t, other)
    order = (q_chunks, q_chunks + 1) + tuple(range(q_chunks))

    def row_of(index, m):
        if m < q_chunks:
            return pl.multiple_of(index * q_rows + m * kv_rows, 8)
        base = shards_in_plane * (q_rows + (m - q_chunks) * kv_rows)
        return pl.multiple_of(base + index * kv_rows, 8)

    def in_weights(at_side, n):
        of_core = core if n < pieces else 1 - core
        return weights.at[pl.ds(row_of(column * tp_size + at_side * 2 + of_core, order[n % pieces]), kv_rows)]

    def in_relay(n):
        return relay.at[pl.ds(n * kv_rows, kv_rows)]

    def in_shard(n):
        return shard.at[pl.ds(order[n] * kv_rows, kv_rows)]

    def place(slot, n):
        return in_weights(side, n) if slot == 0 else in_relay(n)

    def remote(src, dst, send, recv, to_rep, to_tp):
        return pltpu.make_async_remote_copy(
            src_ref=src, dst_ref=dst, send_sem=send, recv_sem=recv,
            device_id=(to_rep, to_tp), device_id_type=MESH,
        )

    def ups(slot):
        k = ranks[slot]
        return (plane >= k) & (plane < planes - 1), (plane <= k) & (plane > 0)

    def x_sends(n, src, dst):
        kind = 0 if n % pieces < 2 else 1
        for d in range(1, columns):
            to = plane * columns + (column + d) % columns
            remote(src, dst, x_send.at[d - 1], x_recv.at[d - 1, kind], to, t).start()

    def forward(slot, n, src, from_source=False):
        up, down = ups(slot)
        if from_source:
            up, down = up & (plane != planes - 2), down & (plane != 1)
        dst = place(slot, n)

        @pl.when(up)
        def _():
            remote(src, dst, z_send.at[slot, 0], z_recv.at[slot, n], r + columns, t).start()

        @pl.when(down)
        def _():
            remote(src, dst, z_send.at[slot, 1], z_recv.at[slot, n], r - columns, t).start()

        if slot == 0:
            x_sends(n, src, dst)
        else:
            remote(src, in_weights(side, n), y_send.at[0], y_recv.at[n], r, other).start()

    def recv_wait(dst, sem):
        remote(dst, dst, x_send.at[0], sem, r, partner).wait_recv()

    def send_wait(src, sem):
        remote(src, src, sem, x_recv.at[0, 0], r, partner).wait_send()

    def source_step(slot, n):
        @pl.when(plane == ranks[slot])
        def _():
            if n < pieces:
                forward(slot, n, in_shard(n), True)
            else:
                recv_wait(place(slot, n), part_recv.at[n - pieces])
                forward(slot, n, place(slot, n), True)

    def late_step(slot, n):
        up, down = ups(slot)
        src, dst = in_shard(n) if n < pieces else place(slot, n), place(slot, n)

        @pl.when((plane == ranks[slot]) & up & (plane == planes - 2))
        def _():
            remote(src, dst, z_send.at[slot, 0], z_recv.at[slot, n], r + columns, t).start()

        @pl.when((plane == ranks[slot]) & down & (plane == 1))
        def _():
            remote(src, dst, z_send.at[slot, 1], z_recv.at[slot, n], r - columns, t).start()

    def relay_step(slot, n):
        @pl.when(plane != ranks[slot])
        def _():
            recv_wait(place(slot, n), z_recv.at[slot, n])
            forward(slot, n, place(slot, n))

    def y_step(n):
        block = in_weights(1 - side, n)
        recv_wait(block, y_recv.at[n])
        x_sends(n, block, block)

    rows = tok.shape[0]

    def prompt_rows(rank):
        return prompts.at[pl.ds(pl.multiple_of(rank * rows, 8), rows)]

    handler = core == plane % 2
    load_shard = pltpu.make_async_copy(shard, shard_buf, local_sem.at[0])
    load_tok = pltpu.make_async_copy(tok, prompt_rows(t), local_sem.at[1])
    load_shard.start()
    load_tok.start()

    @pl.when(jnp.logical_not(handler))
    def _():
        for m in range(pieces):
            @pl.when(side == plane // 2)
            def _():
                dst = weights.at[pl.ds(row_of(column * tp_size + t, order[m]), kv_rows)]
                remote(in_shard(m), dst, part_send.at[0], part_recv.at[m], r, partner).start()

            @pl.when(side != plane // 2)
            def _():
                remote(in_shard(m), in_relay(pieces + m), part_send.at[0], part_recv.at[m], r, partner).start()

    remote(tok, prompt_rows(t), tok_send.at[1], tok_recv.at[1], r, partner).start()

    for n in range(LEAD):
        source_step(0, n)
        source_step(1, n)

    load_shard.wait()
    load_tok.wait()

    def store_shard(m):
        dst = weights.at[pl.ds(row_of(column * tp_size + t, m), kv_rows)]
        return pltpu.make_async_copy(shard_buf.at[pl.ds(m * kv_rows, kv_rows)], dst, local_sem.at[2 + m])

    @pl.when(plane == t)
    def _():
        for m in range(pieces):
            store_shard(m).start()

    late = 0
    for n in range(LATE_FIRST):
        late_step(0, n)
        late_step(1, n)
        late += 1
    for n in range(count):
        if n % LATE_EVERY == LATE_EVERY - 1 and late < count:
            late_step(0, late)
            late_step(1, late)
            late += 1
        if n + LEAD < count:
            source_step(0, n + LEAD)
            source_step(1, n + LEAD)
        relay_step(0, n)
        relay_step(1, n)
        if n == TOK_AT:
            remote(tok, prompt_rows(t), tok_send.at[0], tok_recv.at[0], r, other).start()
        if n >= Y_LAG:
            y_step(n - Y_LAG)
    for n in range(late, count):
        late_step(0, n)
        late_step(1, n)
    for n in range(count - Y_LAG, count):
        y_step(n)
    recv_wait(prompt_rows(other), tok_recv.at[0])
    remote(prompt_rows(other), prompt_rows(other), tok_send.at[2], tok_recv.at[2], r, partner).start()

    recv_wait(prompt_rows(partner), tok_recv.at[1])
    recv_wait(prompt_rows((partner + half) % tp_size), tok_recv.at[2])

    @pl.when(plane == t)
    def _():
        for m in range(pieces):
            store_shard(m).wait()

    block = block_buf.shape[1]
    token_tile = min(256, prompts.shape[0])
    quarter = count * kv_rows
    own = tp_size * q_rows
    firsts = [-(-(c * own) // block) for c in range(columns)]
    early = min((c + 1) * own // block - firsts[c] for c in range(columns))
    early = max(early, 0)
    q_blocks = columns * own // block
    first = (column * own + block - 1) // block

    def load_block(index, at):
        src = weights.at[pl.ds(pl.multiple_of(index * block, block), block)]
        return pltpu.make_async_copy(src, block_buf.at[at], block_sem.at[at])

    def store_block(index, at):
        dst = projected.at[:, pl.ds(pl.multiple_of(index * block, block), block)]
        return pltpu.make_async_copy(result_buf.at[at], dst, result_sem.at[at])

    here = [first + i for i in range(early)] + [q_blocks, q_blocks + 1]
    last = [jnp.where(i >= first, i + early, i) for i in range(q_blocks - early)]
    blocks = here + last

    def multiply(i):
        at = i % 2
        load_block(blocks[i], at).wait()
        if i >= 2:
            store_block(blocks[i - 2], at).wait()

        @pl.loop(0, prompts.shape[0] // token_tile)
        def _(tile):
            at_rows = pl.ds(pl.multiple_of(tile * token_tile, token_tile), token_tile)
            result_buf[at, at_rows, :] = lax.dot_general(
                prompts[at_rows, :], block_buf[at], (((1,), (1,)), ((), ())),
                preferred_element_type=jnp.float32,
            ).astype(result_buf.dtype)

        store_block(blocks[i], at).start()

    kv_part = 2 * 2 * 2 * kv_rows
    if early:
        load_block(blocks[0], 0).start()
    for d in range(1, columns):
        recv_wait(weights.at[pl.ds(0, kv_part)], x_recv.at[d - 1, 0])
    if not early:
        load_block(blocks[0], 0).start()
    for i in range(len(here)):
        if i + 1 < len(here):
            load_block(blocks[i + 1], (i + 1) % 2).start()
        multiply(i)
    for d in range(1, columns):
        recv_wait(weights.at[pl.ds(0, 2 * quarter - kv_part)], x_recv.at[d - 1, 1])
    load_block(blocks[len(here)], len(here) % 2).start()
    for i in range(len(here), len(blocks)):
        if i + 1 < len(blocks):
            load_block(blocks[i + 1], (i + 1) % 2).start()
        multiply(i)
    for i in range(len(blocks) - 2, len(blocks)):
        store_block(blocks[i], i % 2).wait()

    for d in range(1, columns):
        send_wait(weights.at[pl.ds(0, 2 * quarter)], x_send.at[d - 1])
    send_wait(relay, y_send.at[0])
    for slot in range(2):
        for way, go in enumerate(ups(slot)):
            @pl.when(go)
            def _():
                send_wait(relay, z_send.at[slot, way])

    @pl.when(jnp.logical_not(handler))
    def _():
        send_wait(shard, part_send.at[0])

    for i in range(3):
        send_wait(tok, tok_send.at[i])


def gather(shard, tok, q_rows, kv_rows):
    rep_size, tp_size = lax.axis_size("rep"), lax.axis_size("tp")
    columns = rep_size // tp_size
    width = shard.shape[1]
    pieces = q_rows // kv_rows + 2
    count = 2 * pieces
    hbm = pl.BlockSpec(memory_space=pltpu.HBM)
    dma = pltpu.SemaphoreType.DMA
    block = columns * tp_size * kv_rows
    tokens = tp_size * tok.shape[0]
    total = rep_size * shard.shape[0]
    return pl.pallas_call(
        functools.partial(gather_kernel, rep_size, tp_size, q_rows, kv_rows),
        out_shape=(
            jax.ShapeDtypeStruct((total, width), shard.dtype),
            jax.ShapeDtypeStruct((tokens, total), tok.dtype),
        ),
        in_specs=[hbm, hbm],
        out_specs=(hbm, hbm),
        scratch_shapes=[
            pltpu.VMEM((tokens, width), tok.dtype),
            pltpu.VMEM((count * kv_rows, width), shard.dtype),
            pltpu.VMEM(shard.shape, shard.dtype),
            pltpu.VMEM((2, block, width), shard.dtype),
            pltpu.VMEM((2, tokens, block), tok.dtype),
            dma((2 + pieces,)), dma((2,)), dma((2,)),
            dma((1,)), dma((pieces,)),
            dma((2, 2)), dma((2, count)),
            dma((1,)), dma((count,)),
            dma((columns - 1,)), dma((columns - 1, 2)),
            dma((3,)), dma((3,)),
        ],
        compiler_params=pltpu.CompilerParams(has_side_effects=True, vmem_limit_bytes=26 * 2**20),
    )(shard, tok)


def shards(q_weight, key_projection_weight, value_projection_weight, tokens):
    shard = jnp.concatenate(
        [q_weight, key_projection_weight, value_projection_weight], 0
    ).astype(jnp.bfloat16)
    return gather(shard, tokens, q_weight.shape[0], key_projection_weight.shape[0])


def solution(mesh):
    spec = P(("rep", "tp"), None)
    return jax.shard_map(
        shards, mesh=mesh, in_specs=(spec,) * 4, out_specs=(P("tp", None), P("rep", "tp")), check_vma=False
    )
```

```python
import functools

import jax
import jax.numpy as jnp
from jax import lax
from jax.experimental import pallas as pl
from jax.experimental.pallas import tpu as pltpu
from jax.sharding import PartitionSpec as P

MESH = pl.DeviceIdType.MESH
LEAD = 3
Y_LAG = 2
TOK_AT = 11
LATE_FIRST = 1
LATE_EVERY = 2


def gather_kernel(
    rep_size, tp_size, q_rows, kv_rows,
    shard, tok, weights, projected,
    prompts, relay, shard_buf, block_buf, result_buf, local_sem, block_sem, result_sem,
    part_send, part_recv, z_send, z_recv, y_send, y_recv, x_send, x_recv, tok_send, tok_recv,
):
    planes = tp_size
    columns = rep_size // planes
    half = tp_size // 2
    r, t = lax.axis_index("rep"), lax.axis_index("tp")
    plane, column = r // columns, r % columns
    side, core = t // 2, t % 2
    other = (t + half) % tp_size
    partner = t + 1 - 2 * core
    q_chunks = q_rows // kv_rows
    pieces = q_chunks + 2
    count = 2 * pieces
    shards_in_plane = tp_size * columns
    ranks = (t, other)
    order = (q_chunks, q_chunks + 1) + tuple(range(q_chunks))

    def row_of(index, m):
        if m < q_chunks:
            return pl.multiple_of(index * q_rows + m * kv_rows, 8)
        base = shards_in_plane * (q_rows + (m - q_chunks) * kv_rows)
        return pl.multiple_of(base + index * kv_rows, 8)

    def in_weights(at_side, n):
        of_core = core if n < pieces else 1 - core
        return weights.at[pl.ds(row_of(column * tp_size + at_side * 2 + of_core, order[n % pieces]), kv_rows)]

    def in_relay(n):
        return relay.at[pl.ds(n * kv_rows, kv_rows)]

    def in_shard(n):
        return shard.at[pl.ds(order[n] * kv_rows, kv_rows)]

    def place(slot, n):
        return in_weights(side, n) if slot == 0 else in_relay(n)

    def remote(src, dst, send, recv, to_rep, to_tp):
        return pltpu.make_async_remote_copy(
            src_ref=src, dst_ref=dst, send_sem=send, recv_sem=recv,
            device_id=(to_rep, to_tp), device_id_type=MESH,
        )

    def ups(slot):
        k = ranks[slot]
        return (plane >= k) & (plane < planes - 1), (plane <= k) & (plane > 0)

    def x_sends(n, src, dst, which):
        kind = 0 if n % pieces < 2 else 1 + which
        for d in range(1, columns):
            to = plane * columns + (column + d) % columns
            remote(src, dst, x_send.at[d - 1], x_recv.at[d - 1, kind], to, t).start()

    def forward(slot, n, src, from_source=False):
        up, down = ups(slot)
        if from_source:
            up, down = up & (plane != planes - 2), down & (plane != 1)
        dst = place(slot, n)

        @pl.when(up)
        def _():
            remote(src, dst, z_send.at[slot, 0], z_recv.at[slot, n], r + columns, t).start()

        @pl.when(down)
        def _():
            remote(src, dst, z_send.at[slot, 1], z_recv.at[slot, n], r - columns, t).start()

        if slot == 0:
            x_sends(n, src, dst, 0)
        else:
            remote(src, in_weights(side, n), y_send.at[0], y_recv.at[n], r, other).start()

    def recv_wait(dst, sem):
        remote(dst, dst, x_send.at[0], sem, r, partner).wait_recv()

    def send_wait(src, sem):
        remote(src, src, sem, x_recv.at[0, 0], r, partner).wait_send()

    def source_step(slot, n):
        @pl.when(plane == ranks[slot])
        def _():
            if n < pieces:
                forward(slot, n, in_shard(n), True)
            else:
                recv_wait(place(slot, n), part_recv.at[n - pieces])
                forward(slot, n, place(slot, n), True)

    def late_step(slot, n):
        up, down = ups(slot)
        src, dst = in_shard(n) if n < pieces else place(slot, n), place(slot, n)

        @pl.when((plane == ranks[slot]) & up & (plane == planes - 2))
        def _():
            remote(src, dst, z_send.at[slot, 0], z_recv.at[slot, n], r + columns, t).start()

        @pl.when((plane == ranks[slot]) & down & (plane == 1))
        def _():
            remote(src, dst, z_send.at[slot, 1], z_recv.at[slot, n], r - columns, t).start()

    def relay_step(slot, n):
        @pl.when(plane != ranks[slot])
        def _():
            recv_wait(place(slot, n), z_recv.at[slot, n])
            forward(slot, n, place(slot, n))

    def y_step(n):
        block = in_weights(1 - side, n)
        recv_wait(block, y_recv.at[n])
        x_sends(n, block, block, 1)

    rows = tok.shape[0]

    def prompt_rows(rank):
        return prompts.at[pl.ds(pl.multiple_of(rank * rows, 8), rows)]

    handler = core == plane % 2
    load_shard = pltpu.make_async_copy(shard, shard_buf, local_sem.at[0])
    load_tok = pltpu.make_async_copy(tok, prompt_rows(t), local_sem.at[1])
    load_shard.start()
    load_tok.start()

    @pl.when(jnp.logical_not(handler))
    def _():
        for m in range(pieces):
            @pl.when(side == plane // 2)
            def _():
                dst = weights.at[pl.ds(row_of(column * tp_size + t, order[m]), kv_rows)]
                remote(in_shard(m), dst, part_send.at[0], part_recv.at[m], r, partner).start()

            @pl.when(side != plane // 2)
            def _():
                remote(in_shard(m), in_relay(pieces + m), part_send.at[0], part_recv.at[m], r, partner).start()

    remote(tok, prompt_rows(t), tok_send.at[1], tok_recv.at[1], r, partner).start()

    for n in range(LEAD):
        source_step(0, n)
        source_step(1, n)

    load_shard.wait()
    load_tok.wait()

    def store_shard(m):
        dst = weights.at[pl.ds(row_of(column * tp_size + t, m), kv_rows)]
        return pltpu.make_async_copy(shard_buf.at[pl.ds(m * kv_rows, kv_rows)], dst, local_sem.at[2 + m])

    @pl.when(plane == t)
    def _():
        for m in range(pieces):
            store_shard(m).start()

    late = 0
    for n in range(LATE_FIRST):
        late_step(0, n)
        late_step(1, n)
        late += 1
    for n in range(count):
        if n % LATE_EVERY == LATE_EVERY - 1 and late < count:
            late_step(0, late)
            late_step(1, late)
            late += 1
        if n + LEAD < count:
            source_step(0, n + LEAD)
            source_step(1, n + LEAD)
        relay_step(0, n)
        relay_step(1, n)
        if n == TOK_AT:
            remote(tok, prompt_rows(t), tok_send.at[0], tok_recv.at[0], r, other).start()
        if n >= Y_LAG:
            y_step(n - Y_LAG)
    for n in range(late, count):
        late_step(0, n)
        late_step(1, n)
    for n in range(count - Y_LAG, count):
        y_step(n)
    recv_wait(prompt_rows(other), tok_recv.at[0])
    remote(prompt_rows(other), prompt_rows(other), tok_send.at[2], tok_recv.at[2], r, partner).start()

    recv_wait(prompt_rows(partner), tok_recv.at[1])
    recv_wait(prompt_rows((partner + half) % tp_size), tok_recv.at[2])

    @pl.when(plane == t)
    def _():
        for m in range(pieces):
            store_shard(m).wait()

    block = block_buf.shape[1]
    token_tile = min(256, prompts.shape[0])
    quarter = count * kv_rows
    own = tp_size * q_rows
    firsts = [-(-(c * own) // block) for c in range(columns)]
    early = min((c + 1) * own // block - firsts[c] for c in range(columns))
    early = max(early, 0)
    q_blocks = columns * own // block
    first = (column * own + block - 1) // block

    def load_block(index, at):
        src = weights.at[pl.ds(pl.multiple_of(index * block, block), block)]
        return pltpu.make_async_copy(src, block_buf.at[at], block_sem.at[at])

    def store_block(index, at):
        dst = projected.at[:, pl.ds(pl.multiple_of(index * block, block), block)]
        return pltpu.make_async_copy(result_buf.at[at], dst, result_sem.at[at])

    here = [first + i for i in range(early)] + [q_blocks, q_blocks + 1]
    left = q_blocks - early
    places = [jnp.where(side == 0, i, left - 1 - i) for i in range(left)]
    last = [jnp.where(i >= first, i + early, i) for i in places]
    alone = True
    for c in range(columns):
        for s in range(2):
            i = s * (left - 1)
            low = (i + early if i >= firsts[c] else i) * block
            for part in range(low // (2 * q_rows), (low + block - 1) // (2 * q_rows) + 1):
                alone = alone and (part // 2 == c or part % 2 == s)
    blocks = here + last

    def multiply(i):
        at = i % 2
        load_block(blocks[i], at).wait()
        if i >= 2:
            store_block(blocks[i - 2], at).wait()

        @pl.loop(0, prompts.shape[0] // token_tile)
        def _(tile):
            at_rows = pl.ds(pl.multiple_of(tile * token_tile, token_tile), token_tile)
            result_buf[at, at_rows, :] = lax.dot_general(
                prompts[at_rows, :], block_buf[at], (((1,), (1,)), ((), ())),
                preferred_element_type=jnp.float32,
            ).astype(result_buf.dtype)

        store_block(blocks[i], at).start()

    kv_part = 2 * 2 * 2 * kv_rows
    if early:
        load_block(blocks[0], 0).start()
    for d in range(1, columns):
        recv_wait(weights.at[pl.ds(0, kv_part)], x_recv.at[d - 1, 0])
    if not early:
        load_block(blocks[0], 0).start()
    for i in range(len(here)):
        if i + 1 < len(here):
            load_block(blocks[i + 1], (i + 1) % 2).start()
        multiply(i)
    done = len(here)
    for which in (1, 2):
        for d in range(1, columns):
            recv_wait(weights.at[pl.ds(0, quarter - kv_part // 2)], x_recv.at[d - 1, which])
        stop = len(blocks) if which == 2 else done + int(alone)
        for i in range(done, stop):
            if i == done:
                load_block(blocks[i], i % 2).start()
            if i + 1 < stop:
                load_block(blocks[i + 1], (i + 1) % 2).start()
            multiply(i)
        done = stop
    for i in range(len(blocks) - 2, len(blocks)):
        store_block(blocks[i], i % 2).wait()

    for d in range(1, columns):
        send_wait(weights.at[pl.ds(0, 2 * quarter)], x_send.at[d - 1])
    send_wait(relay, y_send.at[0])
    for slot in range(2):
        for way, go in enumerate(ups(slot)):
            @pl.when(go)
            def _():
                send_wait(relay, z_send.at[slot, way])

    @pl.when(jnp.logical_not(handler))
    def _():
        send_wait(shard, part_send.at[0])

    for i in range(3):
        send_wait(tok, tok_send.at[i])


def gather(shard, tok, q_rows, kv_rows):
    rep_size, tp_size = lax.axis_size("rep"), lax.axis_size("tp")
    columns = rep_size // tp_size
    width = shard.shape[1]
    pieces = q_rows // kv_rows + 2
    count = 2 * pieces
    hbm = pl.BlockSpec(memory_space=pltpu.HBM)
    dma = pltpu.SemaphoreType.DMA
    block = columns * tp_size * kv_rows
    tokens = tp_size * tok.shape[0]
    total = rep_size * shard.shape[0]
    return pl.pallas_call(
        functools.partial(gather_kernel, rep_size, tp_size, q_rows, kv_rows),
        out_shape=(
            jax.ShapeDtypeStruct((total, width), shard.dtype),
            jax.ShapeDtypeStruct((tokens, total), tok.dtype),
        ),
        in_specs=[hbm, hbm],
        out_specs=(hbm, hbm),
        scratch_shapes=[
            pltpu.VMEM((tokens, width), tok.dtype),
            pltpu.VMEM((count * kv_rows, width), shard.dtype),
            pltpu.VMEM(shard.shape, shard.dtype),
            pltpu.VMEM((2, block, width), shard.dtype),
            pltpu.VMEM((2, tokens, block), tok.dtype),
            dma((2 + pieces,)), dma((2,)), dma((2,)),
            dma((1,)), dma((pieces,)),
            dma((2, 2)), dma((2, count)),
            dma((1,)), dma((count,)),
            dma((columns - 1,)), dma((columns - 1, 3)),
            dma((3,)), dma((3,)),
        ],
        compiler_params=pltpu.CompilerParams(has_side_effects=True, vmem_limit_bytes=26 * 2**20),
    )(shard, tok)


def shards(q_weight, key_projection_weight, value_projection_weight, tokens):
    shard = jnp.concatenate(
        [q_weight, key_projection_weight, value_projection_weight], 0
    ).astype(jnp.bfloat16)
    return gather(shard, tokens, q_weight.shape[0], key_projection_weight.shape[0])


def solution(mesh):
    spec = P(("rep", "tp"), None)
    return jax.shard_map(
        shards, mesh=mesh, in_specs=(spec,) * 4, out_specs=(P("tp", None), P("rep", "tp")), check_vma=False
    )
```
